256 devices in a mesh: rep: 4 (over y, x), ep: 32 (over z), tp: 2 (over core).
Axes of the slice: x: 2, y: 2, z: 32, core: 2. Of those that a mesh axis runs over, the one named last changes fastest.
The devices are a block of a 4x8x32 slice.
Arguments:
- tokens: bfloat16 [8192, 3072], P(('rep', 'ep')), parts along dimension 0, may hold values from -6 to 6
- routes: int32 [8192, 2], P(('rep', 'ep')), parts along dimension 0, may hold values from 0 to 3, all different within a row; in each aligned block of 64 rows (0 to 63, 64 to 127, ...) at most 40 rows name the same one
- route_weight: float32 [8192, 2], P(('rep', 'ep')), parts along dimension 0, may hold values from 0.2 to 1
- gate_code: bfloat16 [3072, 32768], P(None, ('ep', 'tp')), may hold values from -0.109375 to 0.109375
- gate_scale: float32 [3072, 256], P(None, ('ep', 'tp')), may hold values from 0.5 to 2
- up_code: bfloat16 [3072, 32768], P(None, ('ep', 'tp')), may hold values from -0.109375 to 0.109375
- up_scale: float32 [3072, 256], P(None, ('ep', 'tp')), may hold values from 0.5 to 2
- down_code: bfloat16 [32768, 3072], P(('ep', 'tp')), may hold values from -0.0625 to 0.0625
- down_scale: float32 [32768, 24], P(('ep', 'tp')), may hold values from 0.5 to 2
Outputs:
- mixed: bfloat16 [8192, 3072], P(('rep', 'ep'), 'tp'), parts along dimension 0
The draws below stay inside these ranges and needn't reach their ends.
There are 4 independent parts, one for each index of `rep`. The reference program is written for one: setup_inputs(seed, part) draws one part's arguments, and reference() takes and returns one part's arrays. A program takes and returns all parts, laid end to end along the dimension named above; an argument that names none is the same for every part. Nothing has to cross between parts.
Inputs may be any that keep to these rules, and one draw needn't show every extreme that they name: `routes`: among the 64 rows of one index of ep, no expert is named by more than 40 rows, a bound that some block reaches; a row names 2 different experts.
All inputs are finite; a program needn't handle non-finite values.
Results may differ from the reference program's by a relative error of at most 0.02.
Values may be sent and summed in bfloat16 or wider, within the bound.
No kernel may reach another device: no remote copies, remote signals or barrier semaphores. Data moves between devices by JAX's collectives and lax.ppermute only.
A program may use at most 128 MiB of HBM per device.

```python
import math
import jax
import jax.numpy as jnp
import numpy as np
from jax import lax

D = 3072
FF = 8192
EXPERTS = 4
TOP = 2
QB = 128
TOK_DEV = 64
CAP = 40
TOKENS = 2048
N_EP = 32


def levels(rng, shape, pieces, least, top_value):
    loudness = 1.0
    for axis_at, blocks in pieces:
        heights = jax.random.uniform(jax.random.fold_in(jax.random.fold_in(rng, 6), axis_at), (blocks,), jnp.float32, least / len(pieces), top_value / len(pieces))
        loudness = loudness * jnp.repeat(jnp.exp(heights), shape[axis_at] // blocks).reshape((-1,) + (1,) * (len(shape) - 1 - axis_at))
    return loudness


def deal_out(own_key, own, number, rows, count, top, bound, skew):
    order = jax.random.permutation(own_key, count)
    crowded, usual = load_shares(count, rows * top, bound, skew, True), load_shares(count, rows * top, bound, skew, False)
    places = jnp.arange(count)

    def named(sizes, turn):
        used = int((sizes > 0).sum())
        fixed = max(1, used // 4)
        moved = fixed + (places - fixed + turn * (used - fixed)) % max(1, count - fixed)
        return jnp.zeros((count,), jnp.int32).at[order[jnp.where(places < fixed, places, moved)]].set(jnp.asarray(sizes, jnp.int32))

    sizes = jnp.where(number % 4 == 0, named(crowded, number // 4), named(usual, number - number // 4 - 1))
    mixed = jax.random.permutation(jax.random.fold_in(own, 3), count)
    giver, receiver = mixed[0:count // 2 * 2:2], mixed[1:count // 2 * 2:2]
    slack = jnp.minimum(sizes[giver] - 1, bound - sizes[receiver]) // 2
    slack = jnp.where((giver == order[0]) | (receiver == order[0]) | (sizes[receiver] == 0), 0, jnp.maximum(slack, 0))
    moved = jax.random.randint(jax.random.fold_in(own, 4), (count // 2,), 0, 1 << 20) % (slack + 1)
    sizes = sizes.at[giver].add(-moved).at[receiver].add(moved)
    labels = jnp.searchsorted(jnp.cumsum(sizes), jnp.arange(rows * top), side="right").astype(jnp.int32)
    listing = labels.reshape(top, rows).T
    listing = listing[jax.random.permutation(jax.random.fold_in(own, 1), rows)]
    turn = jax.random.randint(jax.random.fold_in(own, 2), (rows, 1), 0, top)
    return jnp.take_along_axis(listing, (jnp.arange(top)[None, :] + turn) % top, axis=1)


def load_shares(count, total, limit, lean, full):
    loads = [(1 << 20) // math.isqrt(standing ** lean) + 1 for standing in range(1, count + 1)]
    largest = limit if full else min(limit, max(-(-total // count), total * loads[0] // sum(loads)))
    least = 1 if total - largest >= count - 1 else 0
    given, surplus = [largest] + [least] * (count - 1), total - largest - least * (count - 1)
    while surplus > 0:
        movable = [i for i in range(1, count) if given[i] < largest] or [i for i in range(1, count) if given[i] < limit]
        pool, left = sum([loads[i] for i in movable]), surplus
        for i in movable:
            extra = min(limit - given[i], max(1, left * loads[i] // pool), surplus)
            given[i] = given[i] + extra
            surplus = surplus - extra
    return np.array(given)


def scatter_about(key, shape, width, limit, shards=(), held_as=jnp.bfloat16):
    level = levels(key, shape, shards, -0.22, 0.18) if shards else 1.0
    values = jax.random.normal(key, shape, jnp.float32) * width * level
    return jnp.minimum(jnp.maximum(values, -limit), limit).astype(held_as)


def setup_inputs(seed: int = 0, part: int = 0) -> dict:
    key_of = jax.random.split(jax.random.key(seed), 10)
    part_keys = jax.random.split(jax.random.fold_in(key_of[9], part), 10)
    tokens = scatter_about(part_keys[0], (TOKENS, D), 1.0, 6.0, ((0, 32),))
    routes_keys = jax.random.split(jax.random.fold_in(part_keys[1], 1), TOKENS // TOK_DEV)
    routes_turns = jax.random.permutation(jax.random.fold_in(part_keys[1], 3), TOKENS // TOK_DEV)
    routes = jax.vmap(lambda own, number: deal_out(jax.random.fold_in(part_keys[1], 2), own, number, TOK_DEV, EXPERTS, TOP, CAP, 2))(routes_keys, routes_turns).reshape((TOKENS, TOP))
    route_weight = jnp.clip(0.2 + 0.8 * jax.random.uniform(part_keys[2], (TOKENS, TOP), jnp.float32) ** levels(part_keys[2], (TOKENS, TOP), ((0, 32),), -0.2, 0.2), 0.2, 1.0)
    gate_code = scatter_about(key_of[3], (D, EXPERTS * FF), D ** -0.5, 0.109375, ((1, 64),))
    gate_scale = jnp.clip(jnp.exp(math.log(2.0) - 1.3862944 * jax.random.uniform(key_of[4], (D, EXPERTS * FF // QB), jnp.float32) ** levels(key_of[4], (D, EXPERTS * FF // QB), ((1, 64),), -0.2, 0.2)), 0.5, 2.0)
    up_code = scatter_about(key_of[5], (D, EXPERTS * FF), D ** -0.5, 0.109375, ((1, 64),))
    up_scale = jnp.clip(jnp.exp(math.log(2.0) - 1.3862944 * jax.random.uniform(key_of[6], (D, EXPERTS * FF // QB), jnp.float32) ** levels(key_of[6], (D, EXPERTS * FF // QB), ((1, 64),), -0.2, 0.2)), 0.5, 2.0)
    down_code = scatter_about(key_of[7], (EXPERTS * FF, D), FF ** -0.5, 0.0625, ((0, 64),))
    down_scale = jnp.clip(jnp.exp(math.log(2.0) - 1.3862944 * jax.random.uniform(key_of[8], (EXPERTS * FF, D // QB), jnp.float32) ** levels(key_of[8], (EXPERTS * FF, D // QB), ((0, 64),), -0.2, 0.2)), 0.5, 2.0)
    return dict(tokens=tokens, routes=routes, route_weight=route_weight, gate_code=gate_code, gate_scale=gate_scale, up_code=up_code, up_scale=up_scale, down_code=down_code, down_scale=down_scale)


def dequant(code, scale):
    return (code.astype(jnp.float32) * jnp.repeat(scale, QB, axis=1)).astype(jnp.bfloat16)


def slot_table(expert_ids):
    onehot = (expert_ids[:, None] == jnp.arange(EXPERTS, dtype=jnp.int32)[None, :]).astype(jnp.int32)
    before = jnp.cumsum(onehot, axis=0) - onehot
    return jnp.sum(before * onehot, axis=1).astype(jnp.int32)


def reference(tokens, routes, route_weight, gate_code, gate_scale, up_code, up_scale, down_code, down_scale):
    token_blocks = tokens.reshape(N_EP, TOK_DEV, D)
    expert_ids = routes.reshape(N_EP, TOK_DEV * TOP)
    pair_weight = route_weight.reshape(N_EP, TOK_DEV * TOP)
    slot_rank = jax.vmap(slot_table)(expert_ids)
    target = expert_ids * CAP + slot_rank
    columns = jnp.arange(EXPERTS * CAP, dtype=jnp.int32)
    picked = (target[:, None, :] == columns[None, :, None]).astype(jnp.float32)
    repeated = jnp.repeat(token_blocks, TOP, axis=1).astype(jnp.float32)
    buffers = jnp.einsum("scp,spd->scd", picked, repeated).astype(jnp.bfloat16)
    buffers = buffers.reshape(N_EP, EXPERTS, CAP, D)
    outputs = []
    for expert in range(EXPERTS):
        low = expert * FF
        w_gate = dequant(gate_code[:, low:low + FF], gate_scale[:, low // QB:(low + FF) // QB])
        w_up = dequant(up_code[:, low:low + FF], up_scale[:, low // QB:(low + FF) // QB])
        w_down = dequant(down_code[low:low + FF, :], down_scale[low:low + FF, :])
        expert_rows = buffers[:, expert].reshape(N_EP * CAP, D)
        gate_act = jnp.dot(expert_rows, w_gate, preferred_element_type=jnp.float32)
        up_act = jnp.dot(expert_rows, w_up, preferred_element_type=jnp.float32)
        hidden = (jax.nn.silu(gate_act) * up_act).astype(jnp.bfloat16)
        result = jnp.dot(hidden, w_down, preferred_element_type=jnp.float32)
        outputs.append(result.reshape(N_EP, CAP, D))
    stacked = jnp.stack(outputs, axis=1).reshape(N_EP, EXPERTS * CAP, D)
    mixing = jnp.where(target[:, :, None] == columns[None, None, :], pair_weight[:, :, None], 0.0)
    mixing = mixing.astype(jnp.float32).reshape(N_EP, TOK_DEV, TOP, EXPERTS * CAP).sum(axis=2)
    mixed = jnp.einsum("spc,scd->spd", mixing, stacked, precision=lax.Precision.HIGHEST)
    return mixed.reshape(TOKENS, D).astype(jnp.bfloat16)
```

```python
import jax
import jax.numpy as jnp
from jax import lax
from jax.sharding import PartitionSpec as P

EXPERTS = 4
QB = 128
LANES = 128
STREAMS = 2
GROUPS = 4


def dequant(code, scale):
    return (code.astype(jnp.float32) * jnp.repeat(scale, QB, axis=1)).astype(jnp.bfloat16)


def shift(block, axis, by):
    count = lax.axis_size(axis)
    return lax.ppermute(block, axis, [(i, (i + by) % count) for i in range(count)])


def expert_rows(rows, own, other, width, expert):
    x = rows[:, :width]
    hi = rows[:, width : width + EXPERTS].astype(jnp.float32)
    lo = rows[:, width + EXPERTS : width + 2 * EXPERTS].astype(jnp.float32)
    mine = jnp.arange(EXPERTS, dtype=jnp.int32)[None, :] == expert
    weight = jnp.sum(jnp.where(mine, hi + lo, 0.0), axis=1, keepdims=True)
    total = None
    for w_gate, w_up, w_down in (own, other):
        gate_act = jnp.dot(x, w_gate, preferred_element_type=jnp.float32)
        up_act = jnp.dot(x, w_up, preferred_element_type=jnp.float32)
        hidden = (jax.nn.silu(gate_act) * up_act).astype(jnp.bfloat16)
        part = jnp.dot(hidden, w_down, preferred_element_type=jnp.float32)
        total = part if total is None else total + part
    return (total * weight).astype(jnp.bfloat16)


def local(
    tokens, routes, route_weight, gate_code, gate_scale, up_code, up_scale, down_code, down_scale
):
    tok_count, width = tokens.shape
    count = lax.axis_size("ep")
    halves = lax.axis_size("tp")
    core = lax.axis_index("tp")
    expert = lax.axis_index("ep") // (count // EXPERTS)
    rows = tok_count // halves
    piece = rows // STREAMS

    named = routes[:, :, None] == jnp.arange(EXPERTS, dtype=jnp.int32)[None, None, :]
    coef = jnp.sum(jnp.where(named, route_weight[:, :, None], 0.0), axis=1)
    coef_hi = coef.astype(jnp.bfloat16)
    coef_lo = (coef - coef_hi.astype(jnp.float32)).astype(jnp.bfloat16)
    pad = jnp.zeros((tok_count, LANES - 2 * EXPERTS), jnp.bfloat16)
    payload = jnp.concatenate((tokens, coef_hi, coef_lo, pad), axis=1)
    payload = lax.dynamic_slice_in_dim(payload, core * rows, rows, axis=0)

    far = {}
    got = {}
    for stream in range(STREAMS):
        for way in (1, -1):
            odd = (stream + (way < 0)) % 2
            far[way, stream] = count // 2 - odd
            got[way, stream] = [payload[stream * piece : (stream + 1) * piece]]
    for step in range(1, count // 2 + 1):
        for way, stream in got:
            if step <= far[way, stream]:
                got[way, stream].append(shift(got[way, stream][-1], "ep", way))

    own = (dequant(gate_code, gate_scale), dequant(up_code, up_scale), dequant(down_code, down_scale))
    other = tuple(shift(w, "tp", 1) for w in own)

    bounds = [0] + [(count // 2) * (g + 1) // GROUPS for g in range(GROUPS)]
    part = {}
    for g in range(GROUPS):
        first = 0 if g == 0 else bounds[g] + 1
        keys = []
        for step in range(first, bounds[g + 1] + 1):
            for way, stream in got:
                if step <= far[way, stream] and not (step == 0 and way < 0):
                    keys.append((way, stream, step))
        block = jnp.concatenate([got[w, s][d] for w, s, d in keys], axis=0)
        done = expert_rows(block, own, other, width, expert)
        for i, key in enumerate(keys):
            part[key] = done[i * piece : (i + 1) * piece]

    back = {key: part[key[0], key[1], far[key]] for key in got}
    for step in range(count // 2, 0, -1):
        for way, stream in got:
            if step <= far[way, stream]:
                arrived = shift(back[way, stream], "ep", -way)
                if step > 1:
                    summed = arrived.astype(jnp.float32) + part[way, stream, step - 1].astype(jnp.float32)
                    back[way, stream] = summed.astype(jnp.bfloat16)
                else:
                    back[way, stream] = arrived
    mixed = []
    for stream in range(STREAMS):
        total = part[1, stream, 0].astype(jnp.float32)
        for way in (1, -1):
            total = total + back[way, stream].astype(jnp.float32)
        mixed.append(total.astype(jnp.bfloat16))
    mixed = jnp.concatenate(mixed, axis=0)
    return lax.all_to_all(mixed, "tp", split_axis=1, concat_axis=0, tiled=True)


def solution(mesh):
    placed = (
        P(("rep", "ep"), None),
        P(("rep", "ep"), None),
        P(("rep", "ep"), None),
        P(None, ("ep", "tp")),
        P(None, ("ep", "tp")),
        P(None, ("ep", "tp")),
        P(None, ("ep", "tp")),
        P(("ep", "tp"), None),
        P(("ep", "tp"), None),
    )
    return jax.shard_map(
        local, mesh=mesh, in_specs=placed, out_specs=P(("rep", "ep"), "tp"), check_vma=False
    )
```

```python
import functools

import jax
import jax.numpy as jnp
from jax import lax
from jax.experimental import pallas as pl
from jax.experimental.pallas import tpu as pltpu
from jax.sharding import PartitionSpec as P

EXPERTS = 4
QB = 128
LANES = 128
STREAMS = 4
TILE = 8
VMEM = 50 * 1024 * 1024


def dequant_body(*refs):
    third = len(refs) // 3
    for code, scale, out in zip(refs[:third], refs[third : 2 * third], refs[2 * third :]):
        for block in range(code.shape[1] // QB):
            at = slice(block * QB, (block + 1) * QB)
            value = code[:, at].astype(jnp.float32) * scale[:, block : block + 1]
            out[:, at] = value.astype(jnp.bfloat16)


def dequant(codes, scales, rows):
    height, width = codes[0].shape
    tile = pl.BlockSpec((rows, width), lambda i: (i, 0))
    narrow = pl.BlockSpec((rows, width // QB), lambda i: (i, 0))
    return pl.pallas_call(
        dequant_body,
        grid=(height // rows,),
        in_specs=[tile] * len(codes) + [narrow] * len(codes),
        out_specs=[tile] * len(codes),
        out_shape=[jax.ShapeDtypeStruct(c.shape, jnp.bfloat16) for c in codes],
        name="dequant",
    )(*codes, *scales)


def swap(block):
    return lax.ppermute(block, "tp", [(0, 1), (1, 0)])


def hop(block, by, cores=(0, 1)):
    count = lax.axis_size("ep")
    halves = lax.axis_size("tp")
    route = []
    for chip in range(count):
        for core in cores:
            target = (chip + (by if core == 0 else -by)) % count
            route.append((chip * halves + core, target * halves + core))
    return lax.ppermute(block, ("ep", "tp"), route)


def cuts(rows):
    tiles = rows // TILE
    sizes = [(tiles // STREAMS + (s < tiles % STREAMS)) * TILE for s in range(STREAMS)]
    return [(sum(sizes[:s]), sum(sizes[: s + 1])) for s in range(STREAMS)]


def expert_body(far, expert, *refs):
    pieces = refs[: far * STREAMS]
    weights = refs[far * STREAMS : far * STREAMS + 6]
    outs = refs[far * STREAMS + 6 : -1]
    block = refs[-1]
    width = outs[0].shape[1]
    for s, out in enumerate(outs):

        @pl.when(pl.program_id(0) == s)
        def _(s=s, out=out):
            height = out.shape[0]
            for i, piece in enumerate(pieces[s * far : (s + 1) * far]):
                size = piece.shape[0]
                block[i * size : (i + 1) * size, :] = piece[...]
            x = block[:height, :width]
            total = None
            for w_gate, w_up, w_down in (weights[:3], weights[3:]):
                gate_act = jnp.dot(x, w_gate[...], preferred_element_type=jnp.float32)
                up_act = jnp.dot(x, w_up[...], preferred_element_type=jnp.float32)
                hidden = (jax.nn.silu(gate_act) * up_act).astype(jnp.bfloat16)
                part = jnp.dot(hidden, w_down[...], preferred_element_type=jnp.float32)
                total = part if total is None else total + part
            tail = block[:height, width:].astype(jnp.float32)
            lane = lax.broadcasted_iota(jnp.int32, tail.shape, 1)
            mine = (lane == expert[0]) | (lane == expert[0] + EXPERTS)
            weight = jnp.sum(jnp.where(mine, tail, 0.0), axis=1, keepdims=True)
            out[...] = (total * weight).astype(jnp.bfloat16)


def expert_rows(expert, streams, own, other):
    far = len(streams[0])
    width = own[0].shape[0]
    heights = [far * pieces[0].shape[0] for pieces in streams]
    pieces = [piece for stream in streams for piece in stream]
    whole = lambda w: pl.BlockSpec(w.shape, lambda i: (0, 0), pipeline_mode=pl.Buffered(1))
    return pl.pallas_call(
        functools.partial(expert_body, far),
        grid=(STREAMS,),
        in_specs=[pl.BlockSpec(memory_space=pltpu.SMEM)]
        + [whole(w) for w in (*pieces, *own, *other)],
        out_specs=[pl.BlockSpec((h, width), lambda i: (0, 0)) for h in heights],
        out_shape=[jax.ShapeDtypeStruct((h, width), jnp.bfloat16) for h in heights],
        scratch_shapes=[pltpu.VMEM((max(heights), pieces[0].shape[1]), jnp.bfloat16)],
        compiler_params=pltpu.CompilerParams(vmem_limit_bytes=VMEM),
        name="experts",
    )(expert.reshape(1), *pieces, *own, *other)


def local(
    tokens, routes, route_weight, gate_code, gate_scale, up_code, up_scale, down_code, down_scale
):
    tok_count, width = tokens.shape
    count = lax.axis_size("ep")
    upper = lax.axis_index("tp") == 0
    expert = lax.axis_index("ep") // (count // EXPERTS)
    spans = cuts(tok_count)
    far = count // 2

    named = routes[:, :, None] == jnp.arange(EXPERTS, dtype=jnp.int32)[None, None, :]
    coef = jnp.sum(jnp.where(named, route_weight[:, :, None], 0.0), axis=1)
    coef_hi = coef.astype(jnp.bfloat16)
    coef_lo = (coef - coef_hi.astype(jnp.float32)).astype(jnp.bfloat16)
    pad = jnp.zeros((tok_count, LANES - 2 * EXPERTS), jnp.bfloat16)
    payload = jnp.concatenate((tokens, coef_hi, coef_lo, pad), axis=1)

    got = [[payload[first:end] for first, end in spans]]
    for step in range(1, far):
        before, got_now = got[-1], []
        for s in range(STREAMS):
            sending = before[s]
            if step > 2:
                beside = [got[-2][t] for t in range(STREAMS) if t != s]
                sending, *_ = lax.optimization_barrier((sending, *beside))
            got_now.append(hop(sending, 1))
        got.append(got_now)
    last = [hop(rows, 1, (1,)) for rows in got[-1]]
    got.append([jnp.where(upper, mine, rows) for mine, rows in zip(got[0], last)])

    own = []
    for step, code, scale in (
        (1, gate_code, gate_scale),
        (2, up_code, up_scale),
        (3, down_code, down_scale),
    ):
        code, scale, *_ = lax.optimization_barrier((code, scale, *got[step]))
        own += dequant((code,), (scale,), code.shape[0] // 4)
    other = tuple(swap(w) for w in own)

    streams = [[got[d][s] for d in range(1, far + 1)] for s in range(STREAMS)]
    done = expert_rows(expert, streams, own, other)
    part = {
        d: [rows[(d - 1) * (e - f) : d * (e - f)] for rows, (f, e) in zip(done, spans)]
        for d in range(1, far + 1)
    }

    back = [hop(rows, -1, (1,)) for rows in part[far]]
    for step in range(far - 1, 0, -1):
        back = [
            hop((a.astype(jnp.float32) + b.astype(jnp.float32)).astype(jnp.bfloat16), -1)
            for a, b in zip(back, part[step])
        ]
    mixed = jnp.concatenate(
        [
            a.astype(jnp.float32) + jnp.where(upper, b.astype(jnp.float32), 0.0)
            for a, b in zip(back, part[far])
        ],
        axis=0,
    ).astype(jnp.bfloat16)
    halves = lax.axis_size("tp")
    mixed = jnp.moveaxis(mixed.reshape(tok_count, halves, width // halves), 1, 0)
    mixed = lax.all_to_all(mixed, "tp", split_axis=0, concat_axis=0, tiled=True)
    return mixed.astype(jnp.float32).sum(axis=0).astype(jnp.bfloat16)


def solution(mesh):
    placed = (
        P(("rep", "ep"), None),
        P(("rep", "ep"), None),
        P(("rep", "ep"), None),
        P(None, ("ep", "tp")),
        P(None, ("ep", "tp")),
        P(None, ("ep", "tp")),
        P(None, ("ep", "tp")),
        P(("ep", "tp"), None),
        P(("ep", "tp"), None),
    )
    return jax.shard_map(
        local, mesh=mesh, in_specs=placed, out_specs=P(("rep", "ep"), "tp"), check_vma=False
    )
```
